32 devices in a mesh: freq: 8 (over z, core), tm: 4 (over y, x).
Axes of the slice: x: 2, y: 2, z: 4, core: 2. Of those that a mesh axis runs over, the one named last changes fastest.
Arguments:
- band_state: float32 [2048, 4096], P('freq', 'tm'), may hold values from -2.5 to 2.5
- lower_rows: int32 [3, 2048], replicated, may hold values from 0 to 2047, as said below
- upper_rows: int32 [3, 2048], replicated, may hold values from 0 to 2047, as said below
- delays: int32 [3, 2048], replicated, may hold values from 0 to 1024, as said below
- counts: int32 [7], replicated, may hold values from 256 to 2048, as said below
Outputs:
- dedispersed: float32 [2048, 4096], P('freq', 'tm')
The draws below stay inside these ranges and needn't reach their ends.
Inputs may be any that keep to these rules, and one draw needn't show every extreme that they name: `counts`: entry 8 - 8 / 2^k + b is the live row count of output sub-band b of iteration k; it lies between half and all of that sub-band's 2 * 2048 / 2^(3 - k) padded rows, and in every iteration some sub-band has all its rows live. With w = 2048 / 2^(3 - k), lower_rows[k, i] is a row of input sub-band 2 * floor(i / (2 * w)) whose position in that sub-band is below its live count (all w rows are live in iteration 0). With w = 2048 / 2^(3 - k), upper_rows[k, i] is a row of input sub-band 2 * floor(i / (2 * w)) + 1 whose position in that sub-band is below its live count (all w rows are live in iteration 0). delays[k, i] is at most 2048 / 2^(3 - k), and equals it at some row in every iteration.
All inputs are finite; a program needn't handle non-finite values.
Results may differ from the reference program's by a relative error of at most 0.0003.
Values sent between devices are 32-bit elements; how exact they have to be, the bound alone decides.
No kernel may reach another device: no remote copies, remote signals or barrier semaphores. Data moves between devices by JAX's collectives and lax.ppermute only.
A program may use at most 64 MiB of HBM per device.

```python
import jax
import jax.numpy as jnp
from jax import lax

DMAX = 2048
ITERS = 3
NT = 4096


def table_draws(key):
    count_parts = []
    lower_parts = []
    upper_parts = []
    delay_parts = []
    all_rows = jnp.arange(DMAX, dtype=jnp.int32)
    previous = jnp.full((2 ** ITERS,), DMAX >> ITERS, jnp.int32)
    for iteration in range(ITERS):
        width_in = DMAX >> ITERS - iteration
        width_out = 2 * width_in
        bands_out = DMAX // width_out
        level_keys = jax.random.split(jax.random.fold_in(key, 101 + iteration), 6)
        fresh_counts = jax.random.randint(level_keys[0], (bands_out,), width_out // 2, width_out + 1, dtype=jnp.int32)
        full_band = jax.random.randint(level_keys[5], (), 0, bands_out, dtype=jnp.int32)
        fresh_counts = jnp.where(jnp.arange(bands_out, dtype=jnp.int32) == full_band, width_out, fresh_counts)
        band_index = all_rows // width_out
        lower_live = previous[2 * band_index]
        upper_live = previous[2 * band_index + 1]
        lower_pick = jax.random.randint(level_keys[1], (DMAX,), 0, 1 << 30, dtype=jnp.int32) % lower_live
        upper_pick = jax.random.randint(level_keys[2], (DMAX,), 0, 1 << 30, dtype=jnp.int32) % upper_live
        delay_pick = jax.random.randint(level_keys[3], (DMAX,), 0, width_in + 1, dtype=jnp.int32)
        spot_row = jax.random.randint(level_keys[4], (), 0, DMAX, dtype=jnp.int32)
        delay_pick = jnp.where(all_rows == spot_row, width_in, delay_pick)
        count_parts.append(fresh_counts)
        lower_parts.append(2 * band_index * width_in + lower_pick)
        upper_parts.append((2 * band_index + 1) * width_in + upper_pick)
        delay_parts.append(delay_pick)
        previous = fresh_counts
    return (jnp.concatenate(count_parts), jnp.stack(lower_parts), jnp.stack(upper_parts), jnp.stack(delay_parts))


def draw_counts(key, part):
    return table_draws(key)[0]


def draw_lower_rows(key, part):
    return table_draws(key)[1]


def draw_upper_rows(key, part):
    return table_draws(key)[2]


def draw_delays(key, part):
    return table_draws(key)[3]


def block_levels(stream_key, dims, shards, smallest, top_value):
    def one(position, parts):
        draws = jax.random.uniform(jax.random.fold_in(jax.random.fold_in(stream_key, 6), position), (parts,), jnp.float32, smallest / len(shards), top_value / len(shards))
        return jnp.repeat(jnp.exp(draws), dims[position] // parts).reshape((-1,) + (1,) * (len(dims) - position - 1))

    loudness = one(*shards[0])
    for cut in shards[1:]:
        loudness = loudness * one(*cut)
    return loudness


def noise(key, dims, spread, limit, cuts=(), held_as=jnp.bfloat16):
    drawn = spread * jax.random.normal(key, dims, jnp.float32)
    if cuts:
        drawn = drawn * block_levels(key, dims, cuts, -0.22, 0.18)
    return jnp.clip(drawn, -limit, limit).astype(held_as)


def setup_inputs(seed: int = 0) -> dict:
    streams_of = jax.random.split(jax.random.key(seed), 6)
    band_state = noise(streams_of[0], (DMAX, NT), 0.35, 2.5, ((0, 8), (1, 4)), jnp.float32)
    lower_rows = draw_lower_rows(jax.random.fold_in(streams_of[5], 71), 0)
    upper_rows = draw_upper_rows(jax.random.fold_in(streams_of[5], 71), 0)
    delays = draw_delays(jax.random.fold_in(streams_of[5], 71), 0)
    counts = draw_counts(jax.random.fold_in(streams_of[5], 71), 0)
    return {"band_state": band_state, "lower_rows": lower_rows, "upper_rows": upper_rows, "delays": delays, "counts": counts}


def delayed_rows(source_rows, shifts):
    positions = jnp.arange(source_rows.shape[1], dtype=jnp.int32)[None, :] - shifts[:, None]
    picked = jnp.take_along_axis(source_rows, jnp.maximum(positions, 0), axis=1)
    return jnp.where(positions >= 0, picked, jnp.zeros_like(picked))


def reference(band_state, lower_rows, upper_rows, delays, counts):
    block_rows = min(DMAX, 512)
    all_rows = jnp.arange(DMAX, dtype=jnp.int32)
    current = band_state
    for iteration in range(ITERS):
        width_out = DMAX >> (ITERS - iteration - 1)
        offset = 2 ** ITERS - 2 ** (ITERS - iteration)
        live_rows = (all_rows % width_out) < counts[offset + all_rows // width_out]

        def merge_block(pieces, current=current):
            lower_index, upper_index, shifts, keep_rows = pieces
            summed = current[lower_index] + delayed_rows(current[upper_index], shifts)
            return jnp.where(keep_rows[:, None], summed, jnp.zeros_like(summed))

        pieces = (lower_rows[iteration].reshape(-1, block_rows),
                  upper_rows[iteration].reshape(-1, block_rows),
                  delays[iteration].reshape(-1, block_rows),
                  live_rows.reshape(-1, block_rows))
        merged = lax.map(merge_block, pieces)
        current = merged.reshape(DMAX, -1)
    return current
```

```python
from functools import partial

import jax
import jax.numpy as jnp
from jax import lax
from jax.experimental import pallas as pl
from jax.experimental.pallas import tpu as pltpu
from jax.sharding import PartitionSpec as P

DMAX = 2048
ITERS = 3


def shifted_2(block, axis, distance):
    devices = range(lax.axis_size(axis))
    route = [(i - distance, i) for i in devices if i - distance in devices]
    return lax.ppermute(block, axis, route)


def delay_columns(extended, shifts, widest):
    row_count = extended.shape[0]
    for bit_index in range(widest.bit_length()):
        stride = 1 << bit_index
        shifted = jnp.concatenate(
            [jnp.zeros((row_count, stride), extended.dtype), extended[:, :-stride]], axis=1
        )
        extended = jnp.where((shifts >> bit_index & 1)[:, None] == 1, shifted, extended)
    return extended


def live_mask(global_rows, counts, width_out, offset, bands_out):
    band_index = global_rows // width_out
    band_counts = counts[offset : offset + bands_out]
    matches = band_index[:, None] == jnp.arange(bands_out, dtype=jnp.int32)[None, :]
    live_count = jnp.sum(jnp.where(matches, band_counts[None, :], 0), axis=1)
    return global_rows % width_out < live_count


def per_device(band_state, lower_rows, upper_rows, delays, counts):
    row_count, samples = band_state.shape
    freq_index = lax.axis_index("freq")
    first_row = freq_index * row_count
    global_rows = first_row + jnp.arange(row_count, dtype=jnp.int32)
    current = band_state
    for iteration in range(ITERS):
        width_in = DMAX >> ITERS - iteration
        width_out = 2 * width_in
        bands_out = DMAX // width_out
        offset = 2**ITERS - 2 ** (ITERS - iteration)
        lower_source = lax.dynamic_slice_in_dim(lower_rows[iteration], first_row, row_count)
        upper_source = lax.dynamic_slice_in_dim(upper_rows[iteration], first_row, row_count)
        own_delays = lax.dynamic_slice_in_dim(delays[iteration], first_row, row_count)
        gathered = lax.all_gather(current, "freq", axis=0, tiled=True)
        lower_values = jnp.take(gathered, lower_source, axis=0)
        upper_values = jnp.take(gathered, upper_source, axis=0)
        rim_columns = shifted_2(upper_values[:, samples - width_in :], "tm", 1)
        extended = jnp.concatenate([rim_columns, upper_values], axis=1)
        delayed = delay_columns(extended, own_delays, width_in)[:, width_in:]
        live_rows = live_mask(global_rows, counts, width_out, offset, bands_out)
        current = jnp.where(live_rows[:, None], lower_values + delayed, jnp.zeros_like(delayed))
    return current

LANES = 128


def as_index(value, multiple):
    return pl.multiple_of(value, multiple)


def linear_kernel(tail, block, lin, rim):
    rows, samples = block.shape
    pieces = samples // LANES

    def step(group, carry):
        for piece in range(pieces):
            tile = block[pl.ds(as_index(group * 8, 8), 8), piece * LANES : (piece + 1) * LANES]
            lin[pl.ds(group * 8 * pieces + piece, 8, stride=pieces), :] = tile
            if piece >= pieces - tail:
                rim[pl.ds(group * 8 * tail + piece - (pieces - tail), 8, stride=tail), :] = tile
        return carry

    lax.fori_loop(0, rows // 8, step, 0)


def fill(stack, sources, slots, sems):
    size = sources[0].shape[0]
    copies = [
        pltpu.make_async_copy(source, stack.at[pl.ds(as_index(slot * size, 8), size), :], sems.at[n])
        for n, (source, slot) in enumerate(zip(sources, slots))
    ]
    for copy in copies:
        copy.start()
    return copies


def live_limit(where, counts, iteration, rows):
    spread = iteration + 1
    offset = 2**ITERS - 2 ** (ITERS - iteration)
    limit = counts[offset + lax.shift_right_logical(where, spread)]
    return limit - (where & ((1 << spread) - 1)) * rows


def delayed_sum(lower_of, delay_of, extended, pitch, reach, live_rows, row, lanes):
    delay = delay_of(row)
    whole = lax.shift_right_logical(delay, 7)
    part = delay & (LANES - 1)
    start = row * pitch + 8 + reach - whole
    height = pitch - reach
    near = extended[pl.ds(start, height), :]
    past = extended[pl.ds(start - 1, height), :]
    shifted = pltpu.roll(jnp.where(lanes < LANES - part, near, past), part, 1)
    total = lower_of(row) + shifted
    return jnp.where(row < live_rows, total, jnp.zeros_like(total))


def first_kernel(rows, where, counts, lower_rows, upper_rows, delays, own, other, rim, merged, stack, extended, sems):
    height = own.shape[0] // rows
    reach = rim.shape[0] // rows
    pitch = height + reach
    me = where[0]
    copies = fill(stack, (own, other), (me & 1, (me & 1) ^ 1), sems)
    for copy in copies:
        copy.wait()
    base = me * rows
    band = lax.shift_right_logical(me, 1) * (2 * rows)

    def gather(row, carry):
        source = upper_rows[0, base + row] - band
        at = row * pitch + 8
        extended[pl.ds(at, reach), :] = rim[pl.ds((source - rows) * reach, reach), :]
        extended[pl.ds(at + reach, height), :] = stack[pl.ds(as_index(source * height, 8), height), :]
        return carry

    lax.fori_loop(0, rows, gather, 0, unroll=8)
    lanes = lax.broadcasted_iota(jnp.int32, (height, LANES), 1)
    live_rows = live_limit(me, counts, 0, rows)

    def lower_of(row):
        source = lower_rows[0, base + row] - band
        return stack[pl.ds(as_index(source * height, 8), height), :]

    def merge(row, carry):
        merged[pl.ds(as_index(row * height, 8), height), :] = delayed_sum(
            lower_of, lambda r: delays[0, base + r], extended, pitch, reach, live_rows, row, lanes
        )
        return carry

    lax.fori_loop(0, rows, merge, 0, unroll=8)


def pick_near_kernel(rows, iteration, where, lower_rows, upper_rows, a, b, c, d, low, high, rim, stack, sems):
    height = a.shape[0] // rows
    reach = rim.shape[0] // rows
    me = where[0]
    place = me & 3
    copies = fill(stack, (a, b, c, d), (place, place ^ 1, place ^ 2, place ^ 3), sems)
    for copy in copies:
        copy.wait()
    base = me * rows
    band = lax.shift_right_logical(me, 2) * (4 * rows)

    def step(row, carry):
        source = lower_rows[iteration, base + row] - band
        low[pl.ds(as_index(row * height, 8), height), :] = stack[pl.ds(as_index(source * height, 8), height), :]
        source = upper_rows[iteration, base + row] - band
        high[pl.ds(as_index(row * height, 8), height), :] = stack[pl.ds(as_index(source * height, 8), height), :]
        rim[pl.ds(row * reach, reach), :] = stack[pl.ds(source * height + height - reach, reach), :]
        return carry

    lax.fori_loop(0, rows, step, 0, unroll=8)


def pick_half_kernel(rows, iteration, far, where, lower_rows, upper_rows, a, b, c, d, *rest):
    outs, (stack, sems) = rest[:-2], rest[-2:]
    height = a.shape[0] // rows
    me = where[0]
    place = me & 3
    slots = (place ^ 2, place ^ 3, place, place ^ 1) if far else (place, place ^ 1, place ^ 2, place ^ 3)
    copies = fill(stack, (a, b, c, d), slots, sems)
    for copy in copies:
        copy.wait()
    in_upper = lax.shift_right_logical(me, 2) ^ (1 if far else 0)
    band = in_upper * (4 * rows)

    def run(table):
        def step(row, carry):
            for out, base in zip(outs, (me * rows, (me ^ 2) * rows)):
                source = table[iteration, base + row] - band
                out[pl.ds(as_index(row * height, 8), height), :] = stack[
                    pl.ds(as_index(source * height, 8), height), :
                ]
            return carry

        lax.fori_loop(0, rows, step, 0, unroll=8)

    @pl.when(in_upper == 0)
    def _():
        run(lower_rows)

    @pl.when(in_upper == 1)
    def _():
        run(upper_rows)


def join_kernel(rows, iteration, last, where, counts, delays, low, high, rim, merged, extended, *more):
    height = low.shape[0] // rows
    reach = rim.shape[0] // rows
    pitch = height + reach
    me = where[0]
    base = me * rows

    def gather(row, carry):
        at = row * pitch + 8
        extended[pl.ds(at, reach), :] = rim[pl.ds(row * reach, reach), :]
        extended[pl.ds(at + reach, height), :] = high[pl.ds(as_index(row * height, 8), height), :]
        return carry

    lax.fori_loop(0, rows, gather, 0, unroll=8)
    lanes = lax.broadcasted_iota(jnp.int32, (height, LANES), 1)
    live_rows = live_limit(me, counts, iteration, rows)
    target = more[0] if last else merged

    def merge(row, carry):
        target[pl.ds(as_index(row * height, 8), height), :] = delayed_sum(
            lambda r: low[pl.ds(as_index(r * height, 8), height), :],
            lambda r: delays[iteration, base + r], extended, pitch, reach, live_rows, row, lanes,
        )
        return carry

    lax.fori_loop(0, rows, merge, 0, unroll=8)
    if last:
        def step(group, carry):
            for piece in range(height):
                merged[pl.ds(as_index(group * 8, 8), 8), piece * LANES : (piece + 1) * LANES] = target[
                    pl.ds(group * 8 * height + piece, 8, stride=height), :
                ]
            return carry

        lax.fori_loop(0, rows // 8, step, 0)


SMEM = pl.BlockSpec(memory_space=pltpu.SMEM)
VMEM = pl.BlockSpec(memory_space=pltpu.VMEM)
HBM = pl.BlockSpec(memory_space=pl.ANY)


def f32(*shape):
    return jax.ShapeDtypeStruct(shape, jnp.float32)


def scratch(*shape):
    return pltpu.VMEM(shape, jnp.float32)


def call(kernel, ins, outs, scratches, *args):
    return pl.pallas_call(
        kernel,
        in_specs=list(ins),
        out_specs=[VMEM] * len(outs),
        out_shape=list(outs),
        scratch_shapes=list(scratches),
    )(*args)


def hop(block, pairs):
    return lax.ppermute(block, "freq", pairs)


def merged_by_chips(band_state, lower_rows, upper_rows, delays, counts):
    rows, samples = band_state.shape
    height = samples // LANES
    size = rows * height
    devices = lax.axis_size("freq")
    steps = lax.axis_size("tm")
    where = lax.axis_index("freq").astype(jnp.int32)[None]
    everyone = range(devices)

    def twist(block, bits):
        return hop(block, [(i, i ^ bits) for i in everyone])

    def onward(block):
        return lax.ppermute(block, "tm", [(t, t + 1) for t in range(steps - 1)])

    reach = rows // LANES
    lin, tail = call(
        partial(linear_kernel, reach), [VMEM], [f32(size, LANES), f32(rows * reach, LANES)], [], band_state
    )
    other = twist(lin, 1)
    grid = [(f, t) for f in everyone if f % 2 for t in range(steps - 1)]
    straight = [(f * steps + t, f * steps + t + 1) for f, t in grid]
    across = [(f * steps + t, (f - 1) * steps + t + 1) for f, t in grid]
    rim_odd = lax.ppermute(tail, ("freq", "tm"), straight)
    rim_even = lax.ppermute(tail, ("freq", "tm"), across)
    rim = rim_odd + rim_even
    (current,) = call(
        partial(first_kernel, rows),
        [SMEM] * 5 + [HBM] * 2 + [VMEM],
        [f32(size, LANES)],
        [scratch(2 * size, LANES), scratch(rows * (height + reach) + 16, LANES), pltpu.SemaphoreType.DMA((2,))],
        where, counts, lower_rows, upper_rows, delays, lin, other, rim,
    )

    reach = 2 * reach
    beside = twist(current, 1)
    over = twist(current, 2)
    diagonal = twist(over, 1)
    stacked = [scratch(4 * size, LANES), pltpu.SemaphoreType.DMA((4,))]
    low, high, rim = call(
        partial(pick_near_kernel, rows, 1),
        [SMEM] * 3 + [HBM] * 4,
        [f32(size, LANES), f32(size, LANES), f32(rows * reach, LANES)],
        stacked,
        where, lower_rows, upper_rows, current, beside, over, diagonal,
    )
    (current,) = call(
        partial(join_kernel, rows, 1, False),
        [SMEM] * 3 + [VMEM] * 3,
        [f32(size, LANES)],
        [scratch(rows * (height + reach) + 16, LANES)],
        where, counts, delays, low, high, onward(rim),
    )

    reach = 2 * reach
    inner = hop(current, [(i, i ^ 6) for i in everyone if i & 2 != i >> 1 & 2])
    outer = hop(current, [(i, i ^ 4) for i in everyone if i & 2 == i >> 1 & 2])
    over = twist(current, 2)
    beside = twist(current, 1)
    inner_beside = twist(inner, 1)
    outer_beside = twist(outer, 1)
    diagonal = twist(over, 1)
    (near,) = call(
        partial(pick_half_kernel, rows, 2, False),
        [SMEM] * 3 + [HBM] * 4, [f32(size, LANES)], stacked,
        where, lower_rows, upper_rows, current, beside, over, diagonal,
    )
    far_own, far_next = call(
        partial(pick_half_kernel, rows, 2, True),
        [SMEM] * 3 + [HBM] * 4, [f32(size, LANES)] * 2, stacked,
        where, lower_rows, upper_rows, inner, inner_beside, outer, outer_beside,
    )
    hub = where[0] & 2 != where[0] >> 1 & 2
    handed = hop(far_next, [(i, i ^ 2) for i in everyone if i & 2 != i >> 1 & 2])
    far = jnp.where(hub, far_own, handed)
    in_upper = where[0] >> 2 == 1
    low = jnp.where(in_upper, far, near)
    high = jnp.where(in_upper, near, far)
    (merged,) = call(
        partial(join_kernel, rows, 2, True),
        [SMEM] * 3 + [VMEM] * 3,
        [f32(rows, samples)],
        [scratch(rows * (height + reach) + 16, LANES), scratch(size, LANES)],
        where, counts, delays, low, high, onward(high),
    )
    return merged


def solution(mesh):
    def body(band_state, *tables):
        rows, samples = band_state.shape
        fits = rows == DMAX >> ITERS and rows % LANES == 0 and samples == 8 * LANES
        if ITERS == 3 and fits:
            return merged_by_chips(band_state, *tables)
        return per_device(band_state, *tables)

    return jax.shard_map(
        body,
        mesh=mesh,
        in_specs=(P("freq", "tm"), P(), P(), P(), P()),
        out_specs=P("freq", "tm"),
        check_vma=False,
    )
```

```python
from functools import partial

import jax
import jax.numpy as jnp
from jax import lax
from jax.experimental import pallas as pl
from jax.experimental.pallas import tpu as pltpu
from jax.sharding import PartitionSpec as P

DMAX = 2048
ITERS = 3


def shifted_2(block, axis, distance):
    devices = range(lax.axis_size(axis))
    route = [(i - distance, i) for i in devices if i - distance in devices]
    return lax.ppermute(block, axis, route)


def delay_columns(extended, shifts, widest):
    row_count = extended.shape[0]
    for bit_index in range(widest.bit_length()):
        stride = 1 << bit_index
        shifted = jnp.concatenate(
            [jnp.zeros((row_count, stride), extended.dtype), extended[:, :-stride]], axis=1
        )
        extended = jnp.where((shifts >> bit_index & 1)[:, None] == 1, shifted, extended)
    return extended


def live_mask(global_rows, counts, width_out, offset, bands_out):
    band_index = global_rows // width_out
    band_counts = counts[offset : offset + bands_out]
    matches = band_index[:, None] == jnp.arange(bands_out, dtype=jnp.int32)[None, :]
    live_count = jnp.sum(jnp.where(matches, band_counts[None, :], 0), axis=1)
    return global_rows % width_out < live_count


def per_device(band_state, lower_rows, upper_rows, delays, counts):
    row_count, samples = band_state.shape
    freq_index = lax.axis_index("freq")
    first_row = freq_index * row_count
    global_rows = first_row + jnp.arange(row_count, dtype=jnp.int32)
    current = band_state
    for iteration in range(ITERS):
        width_in = DMAX >> ITERS - iteration
        width_out = 2 * width_in
        bands_out = DMAX // width_out
        offset = 2**ITERS - 2 ** (ITERS - iteration)
        lower_source = lax.dynamic_slice_in_dim(lower_rows[iteration], first_row, row_count)
        upper_source = lax.dynamic_slice_in_dim(upper_rows[iteration], first_row, row_count)
        own_delays = lax.dynamic_slice_in_dim(delays[iteration], first_row, row_count)
        gathered = lax.all_gather(current, "freq", axis=0, tiled=True)
        lower_values = jnp.take(gathered, lower_source, axis=0)
        upper_values = jnp.take(gathered, upper_source, axis=0)
        rim_columns = shifted_2(upper_values[:, samples - width_in :], "tm", 1)
        extended = jnp.concatenate([rim_columns, upper_values], axis=1)
        delayed = delay_columns(extended, own_delays, width_in)[:, width_in:]
        live_rows = live_mask(global_rows, counts, width_out, offset, bands_out)
        current = jnp.where(live_rows[:, None], lower_values + delayed, jnp.zeros_like(delayed))
    return current

LANES = 128


def as_index(value, multiple):
    return pl.multiple_of(value, multiple)


def linear_kernel(tail, block, lin, rim):
    rows, samples = block.shape
    pieces = samples // LANES

    def step(group, carry):
        for piece in range(pieces):
            tile = block[pl.ds(as_index(group * 8, 8), 8), piece * LANES : (piece + 1) * LANES]
            lin[pl.ds(group * 8 * pieces + piece, 8, stride=pieces), :] = tile
            if piece >= pieces - tail:
                rim[pl.ds(group * 8 * tail + piece - (pieces - tail), 8, stride=tail), :] = tile
        return carry

    lax.fori_loop(0, rows // 8, step, 0)


def fill(stack, sources, slots, sems):
    size = sources[0].shape[0]
    copies = [
        pltpu.make_async_copy(source, stack.at[pl.ds(as_index(slot * size, 8), size), :], sems.at[n])
        for n, (source, slot) in enumerate(zip(sources, slots))
    ]
    for copy in copies:
        copy.start()
    return copies


def live_limit(where, counts, iteration, rows):
    spread = iteration + 1
    offset = 2**ITERS - 2 ** (ITERS - iteration)
    limit = counts[offset + lax.shift_right_logical(where, spread)]
    return limit - (where & ((1 << spread) - 1)) * rows


def move(target, to, source, start, height):
    target[pl.ds(to, height), :] = source[pl.ds(start, height), :]


def add_delayed(rows, iteration, table, live_rows, extended, lowered, put):
    lanes = lax.broadcasted_iota(jnp.int32, (8, LANES), 1)

    def merge(row, carry):
        delay = table[(2 * ITERS + iteration) * rows + row]
        start = row * 16 + 16 - lax.shift_right_logical(delay, 7)
        part = delay & (LANES - 1)
        near = extended[pl.ds(start, 8), :]
        past = extended[pl.ds(start - 1, 8), :]
        shifted = pltpu.roll(jnp.where(lanes < LANES - part, near, past), part, 1)
        total = lowered(row) + shifted
        put(row, jnp.where(row < live_rows, total, jnp.zeros_like(total)))
        return carry

    lax.fori_loop(0, rows, merge, 0, unroll=8)


def put_halves(first, second):
    def put(row, total):
        first[pl.ds(as_index(row * 4, 4), 4), :] = total[:4]
        second[pl.ds(as_index(row * 4, 4), 4), :] = total[4:]

    return put


def first_kernel(rows, where, counts, table, own, other, rim, first, second, stack, extended, sems):
    reach = rim.shape[0] // rows
    me = where[0]
    copies = fill(stack, (own, other), (me & 1, (me & 1) ^ 1), sems)
    for copy in copies:
        copy.wait()
    band = lax.shift_right_logical(me, 1) * (2 * rows)

    def gather(row, carry):
        source = table[ITERS * rows + row] - band
        move(extended, row * 16 + 16 - reach, rim, (source - rows) * reach, reach)
        move(extended, as_index(row * 16 + 16, 8), stack, as_index(source * 8, 8), 8)
        return carry

    lax.fori_loop(0, rows, gather, 0, unroll=8)

    def lowered(row):
        return stack[pl.ds(as_index((table[row] - band) * 8, 8), 8), :]

    add_delayed(rows, 0, table, live_limit(me, counts, 0, rows), extended, lowered, put_halves(first, second))


def places(me, far):
    place = me & 3
    return (place ^ 2, place ^ 3, place, place ^ 1) if far else (place, place ^ 1, place ^ 2, place ^ 3)


def pick_rim_kernel(rows, where, table, a, b, c, d, rim, stack, sems):
    me = where[0]
    for copy in fill(stack, (a, b, c, d), places(me, False), sems):
        copy.wait()
    band = lax.shift_right_logical(me, 2) * (4 * rows)

    def step(row, carry):
        source = table[(ITERS + 1) * rows + row] - band
        move(rim, as_index(row * 4, 4), stack, as_index(source * 4, 4), 4)
        return carry

    lax.fori_loop(0, rows, step, 0, unroll=8)


def pick_pair_kernel(rows, where, table, *refs):
    low, high, stack, sems = refs[8:]
    me = where[0]
    size = 4 * refs[0].shape[0]
    slots = places(me, False)
    copies = fill(stack.at[pl.ds(0, size), :], refs[:4], slots, sems.at[0])
    copies += fill(stack.at[pl.ds(size, size), :], refs[4:8], slots, sems.at[1])
    for copy in copies:
        copy.wait()
    band = lax.shift_right_logical(me, 2) * (4 * rows)

    def step(row, carry):
        for out, entry in ((low, rows), (high, (ITERS + 1) * rows)):
            source = (table[entry + row] - band) * 4
            move(out, as_index(row * 8, 8), stack, as_index(source, 4), 4)
            move(out, as_index(row * 8, 8) + 4, stack, size + source, 4)
        return carry

    lax.fori_loop(0, rows, step, 0, unroll=8)


def pick_half_kernel(rows, far, where, *refs):
    count = 2 if far else 1
    tables, sources, outs = refs[:count], refs[count : count + 4], refs[count + 4 : -2]
    stack, sems = refs[-2:]
    me = where[0]
    for copy in fill(stack, sources, places(me, far), sems):
        copy.wait()
    in_upper = lax.shift_right_logical(me, 2) ^ (1 if far else 0)
    band = in_upper * (4 * rows)
    entry = (in_upper * ITERS + 2) * rows

    def step(row, carry):
        for out, table in zip(outs, tables):
            source = (table[entry + row] - band) * 4
            move(out, as_index(row * 4, 4), stack, as_index(source, 4), 4)
        return carry

    lax.fori_loop(0, rows, step, 0, unroll=8)


def second_kernel(rows, where, counts, table, low, high, rim, first, second, extended):
    me = where[0]

    def gather(row, carry):
        move(extended, row * 16 + 12, rim, as_index(row * 4, 4), 4)
        move(extended, as_index(row * 16 + 16, 8), high, as_index(row * 8, 8), 8)
        return carry

    lax.fori_loop(0, rows, gather, 0, unroll=8)

    def lowered(row):
        return low[pl.ds(as_index(row * 8, 8), 8), :]

    add_delayed(rows, 1, table, live_limit(me, counts, 1, rows), extended, lowered, put_halves(first, second))


def last_kernel(rows, where, counts, table, low_a, low_b, high_a, high_b, rim_a, rim_b, merged, extended, low, lin):
    me = where[0]

    def gather(row, carry):
        for n, piece in enumerate((rim_a, rim_b, high_a, high_b)):
            move(extended, as_index(row * 16 + 8, 8) + n * 4, piece, as_index(row * 4, 4), 4)
        for n, piece in enumerate((low_a, low_b)):
            move(low, as_index(row * 8, 8) + n * 4, piece, as_index(row * 4, 4), 4)
        return carry

    lax.fori_loop(0, rows, gather, 0, unroll=8)

    def lowered(row):
        return low[pl.ds(as_index(row * 8, 8), 8), :]

    def put(row, total):
        lin[pl.ds(as_index(row * 8, 8), 8), :] = total

    add_delayed(rows, 2, table, live_limit(me, counts, 2, rows), extended, lowered, put)

    def step(group, carry):
        for piece in range(8):
            merged[pl.ds(as_index(group * 8, 8), 8), piece * LANES : (piece + 1) * LANES] = lin[
                pl.ds(group * 64 + piece, 8, stride=8), :
            ]
        return carry

    lax.fori_loop(0, rows // 8, step, 0, unroll=2)


SMEM = pl.BlockSpec(memory_space=pltpu.SMEM)
VMEM = pl.BlockSpec(memory_space=pltpu.VMEM)
HBM = pl.BlockSpec(memory_space=pl.ANY)


def f32(*shape):
    return jax.ShapeDtypeStruct(shape, jnp.float32)


def scratch(*shape):
    return pltpu.VMEM(shape, jnp.float32)


def call(kernel, ins, outs, scratches, *args):
    return pl.pallas_call(
        kernel,
        in_specs=list(ins),
        out_specs=[VMEM] * len(outs),
        out_shape=list(outs),
        scratch_shapes=list(scratches),
    )(*args)


def hop(block, pairs):
    return lax.ppermute(block, "freq", pairs)


def merged_by_chips(band_state, lower_rows, upper_rows, delays, counts):
    rows, samples = band_state.shape
    size = rows * (samples // LANES)
    half = size // 2
    devices = lax.axis_size("freq")
    steps = lax.axis_size("tm")
    me = lax.axis_index("freq").astype(jnp.int32)
    where = me[None]
    everyone = range(devices)
    hubs = [i for i in everyone if i & 2 != i >> 1 & 2]
    edges = [i for i in everyone if i not in hubs]

    def twist(block, bits):
        return hop(block, [(i, i ^ bits) for i in everyone])

    def onward(block):
        return lax.ppermute(block, "tm", [(t, t + 1) for t in range(steps - 1)])

    reach = rows // LANES
    lin, tail = call(
        partial(linear_kernel, reach), [VMEM], [f32(size, LANES), f32(rows * reach, LANES)], [], band_state
    )
    other = twist(lin, 1)
    grid = [(f, t) for f in everyone if f % 2 for t in range(steps - 1)]
    straight = [(f * steps + t, f * steps + t + 1) for f, t in grid]
    across = [(f * steps + t, (f - 1) * steps + t + 1) for f, t in grid]
    rim_odd = lax.ppermute(tail, ("freq", "tm"), straight)
    rim_even = lax.ppermute(tail, ("freq", "tm"), across)
    tables = jnp.concatenate([lower_rows, upper_rows, delays], axis=0)

    def own_table(device):
        return lax.dynamic_slice_in_dim(tables, device * rows, rows, axis=1).reshape(-1)

    table = own_table(me)
    table_over = own_table(me ^ 2)
    extended = scratch(rows * 16 + 16, LANES)
    halves = [f32(half, LANES)] * 2
    first, second = call(
        partial(first_kernel, rows),
        [SMEM] * 3 + [HBM] * 2 + [VMEM],
        halves,
        [scratch(2 * size, LANES), extended, pltpu.SemaphoreType.DMA((2,))],
        where, counts, table, lin, other, rim_odd + rim_even,
    )

    over_b = twist(second, 2)
    over_a = twist(first, 2)
    near_b = (second, twist(second, 1), over_b, twist(over_b, 1))
    near_a = (first, twist(first, 1), over_a, twist(over_a, 1))
    stacked = [scratch(4 * half, LANES), pltpu.SemaphoreType.DMA((4,))]
    (rim,) = call(
        partial(pick_rim_kernel, rows), [SMEM] * 2 + [HBM] * 4, [f32(half, LANES)], stacked, where, table, *near_b
    )
    rim = onward(rim)
    low, high = call(
        partial(pick_pair_kernel, rows),
        [SMEM] * 2 + [HBM] * 8,
        [f32(size, LANES)] * 2,
        [scratch(8 * half, LANES), pltpu.SemaphoreType.DMA((2, 4))],
        where, table, *near_a, *near_b,
    )
    first, second = call(
        partial(second_kernel, rows), [SMEM] * 3 + [VMEM] * 3, halves, [extended], where, counts, table, low, high, rim
    )

    hub = me & 2 != me >> 1 & 2
    in_upper = me >> 2 == 1

    def selected(block):
        inner = hop(block, [(i, i ^ 6) for i in hubs])
        outer = hop(block, [(i, i ^ 4) for i in edges])
        over = twist(block, 2)
        (near,) = call(
            partial(pick_half_kernel, rows, False),
            [SMEM] * 2 + [HBM] * 4, [f32(half, LANES)], stacked,
            where, table, block, twist(block, 1), over, twist(over, 1),
        )
        far_own, far_next = call(
            partial(pick_half_kernel, rows, True),
            [SMEM] * 3 + [HBM] * 4, halves, stacked,
            where, table, table_over, inner, twist(inner, 1), outer, twist(outer, 1),
        )
        far = jnp.where(hub, far_own, hop(far_next, [(i, i ^ 2) for i in hubs]))
        high = jnp.where(in_upper, near, far)
        return jnp.where(in_upper, far, near), high, onward(high)

    low_b, high_b, rim_b = selected(second)
    low_a, high_a, rim_a = selected(first)
    (merged,) = call(
        partial(last_kernel, rows),
        [SMEM] * 3 + [VMEM] * 6,
        [f32(rows, samples)],
        [extended, scratch(size, LANES), scratch(size, LANES)],
        where, counts, table, low_a, low_b, high_a, high_b, rim_a, rim_b,
    )
    return merged


def solution(mesh):
    def body(band_state, *tables):
        rows, samples = band_state.shape
        fits = rows == DMAX >> ITERS and rows % LANES == 0 and samples == 8 * LANES
        if ITERS == 3 and fits:
            return merged_by_chips(band_state, *tables)
        return per_device(band_state, *tables)

    return jax.shard_map(
        body,
        mesh=mesh,
        in_specs=(P("freq", "tm"), P(), P(), P(), P()),
        out_specs=P("freq", "tm"),
        check_vma=False,
    )
```

```python
from functools import partial

import jax
import jax.numpy as jnp
from jax import lax
from jax.experimental import pallas as pl
from jax.experimental.pallas import tpu as pltpu
from jax.sharding import PartitionSpec as P

DMAX = 2048
ITERS = 3


def shifted_2(block, axis, distance):
    devices = range(lax.axis_size(axis))
    route = [(i - distance, i) for i in devices if i - distance in devices]
    return lax.ppermute(block, axis, route)


def delay_columns(extended, shifts, widest):
    row_count = extended.shape[0]
    for bit_index in range(widest.bit_length()):
        stride = 1 << bit_index
        shifted = jnp.concatenate(
            [jnp.zeros((row_count, stride), extended.dtype), extended[:, :-stride]], axis=1
        )
        extended = jnp.where((shifts >> bit_index & 1)[:, None] == 1, shifted, extended)
    return extended


def live_mask(global_rows, counts, width_out, offset, bands_out):
    band_index = global_rows // width_out
    band_counts = counts[offset : offset + bands_out]
    matches = band_index[:, None] == jnp.arange(bands_out, dtype=jnp.int32)[None, :]
    live_count = jnp.sum(jnp.where(matches, band_counts[None, :], 0), axis=1)
    return global_rows % width_out < live_count


def per_device(band_state, lower_rows, upper_rows, delays, counts):
    row_count, samples = band_state.shape
    freq_index = lax.axis_index("freq")
    first_row = freq_index * row_count
    global_rows = first_row + jnp.arange(row_count, dtype=jnp.int32)
    current = band_state
    for iteration in range(ITERS):
        width_in = DMAX >> ITERS - iteration
        width_out = 2 * width_in
        bands_out = DMAX // width_out
        offset = 2**ITERS - 2 ** (ITERS - iteration)
        lower_source = lax.dynamic_slice_in_dim(lower_rows[iteration], first_row, row_count)
        upper_source = lax.dynamic_slice_in_dim(upper_rows[iteration], first_row, row_count)
        own_delays = lax.dynamic_slice_in_dim(delays[iteration], first_row, row_count)
        gathered = lax.all_gather(current, "freq", axis=0, tiled=True)
        lower_values = jnp.take(gathered, lower_source, axis=0)
        upper_values = jnp.take(gathered, upper_source, axis=0)
        rim_columns = shifted_2(upper_values[:, samples - width_in :], "tm", 1)
        extended = jnp.concatenate([rim_columns, upper_values], axis=1)
        delayed = delay_columns(extended, own_delays, width_in)[:, width_in:]
        live_rows = live_mask(global_rows, counts, width_out, offset, bands_out)
        current = jnp.where(live_rows[:, None], lower_values + delayed, jnp.zeros_like(delayed))
    return current


LANES = 128


def as_index(value, multiple):
    return pl.multiple_of(value, multiple)


def linear_kernel(tail, block, lin, rim):
    rows, samples = block.shape
    pieces = samples // LANES

    def step(group, carry):
        for piece in range(pieces):
            tile = block[pl.ds(as_index(group * 8, 8), 8), piece * LANES : (piece + 1) * LANES]
            lin[pl.ds(group * 8 * pieces + piece, 8, stride=pieces), :] = tile
            if piece >= pieces - tail:
                rim[pl.ds(group * 8 * tail + piece - (pieces - tail), 8, stride=tail), :] = tile
        return carry

    lax.fori_loop(0, rows // 8, step, 0)


def fill(stack, sources, slots, sems):
    size = sources[0].shape[0]
    copies = [
        pltpu.make_async_copy(source, stack.at[pl.ds(as_index(slot * size, 8), size), :], sems.at[n])
        for n, (source, slot) in enumerate(zip(sources, slots))
    ]
    for copy in copies:
        copy.start()
    return copies


def live_limit(where, counts, iteration, rows):
    spread = iteration + 1
    offset = 2**ITERS - 2 ** (ITERS - iteration)
    limit = counts[offset + lax.shift_right_logical(where, spread)]
    return limit - (where & ((1 << spread) - 1)) * rows


def move(target, to, source, start, height):
    target[pl.ds(to, height), :] = source[pl.ds(start, height), :]


def add_delayed(rows, iteration, table, live_rows, extended, lowered, put):
    lanes = lax.broadcasted_iota(jnp.int32, (8, LANES), 1)

    def merge(row, carry):
        delay = table[(2 * ITERS + iteration) * rows + row]
        start = row * 16 + 16 - lax.shift_right_logical(delay, 7)
        part = delay & (LANES - 1)
        near = extended[pl.ds(start, 8), :]
        past = extended[pl.ds(start - 1, 8), :]
        shifted = pltpu.roll(jnp.where(lanes < LANES - part, near, past), part, 1)
        total = lowered(row) + shifted
        put(row, jnp.where(row < live_rows, total, jnp.zeros_like(total)))
        return carry

    lax.fori_loop(0, rows, merge, 0, unroll=8)


def put_halves(first, second):
    def put(row, total):
        first[pl.ds(as_index(row * 4, 4), 4), :] = total[:4]
        second[pl.ds(as_index(row * 4, 4), 4), :] = total[4:]

    return put


def first_kernel(rows, where, counts, table, own, other, rim, first, second, stack, extended, sems):
    reach = rim.shape[0] // rows
    me = where[0]
    copies = fill(stack, (own, other), (me & 1, (me & 1) ^ 1), sems)
    for copy in copies:
        copy.wait()
    band = lax.shift_right_logical(me, 1) * (2 * rows)

    def gather(row, carry):
        source = table[ITERS * rows + row] - band
        move(extended, row * 16 + 16 - reach, rim, (source - rows) * reach, reach)
        move(extended, as_index(row * 16 + 16, 8), stack, as_index(source * 8, 8), 8)
        return carry

    lax.fori_loop(0, rows, gather, 0, unroll=8)

    def lowered(row):
        return stack[pl.ds(as_index((table[row] - band) * 8, 8), 8), :]

    add_delayed(rows, 0, table, live_limit(me, counts, 0, rows), extended, lowered, put_halves(first, second))


def places(me, far):
    place = me & 3
    return (place ^ 2, place ^ 3, place, place ^ 1) if far else (place, place ^ 1, place ^ 2, place ^ 3)


def pick_rim_kernel(rows, where, table, a, b, c, d, rim, stack, sems):
    me = where[0]
    for copy in fill(stack, (a, b, c, d), places(me, False), sems):
        copy.wait()
    band = lax.shift_right_logical(me, 2) * (4 * rows)

    def step(row, carry):
        source = table[(ITERS + 1) * rows + row] - band
        move(rim, as_index(row * 4, 4), stack, as_index(source * 4, 4), 4)
        return carry

    lax.fori_loop(0, rows, step, 0, unroll=8)


def pick_pair_kernel(rows, where, table, *refs):
    low, high, stack, sems = refs[8:]
    me = where[0]
    size = 4 * refs[0].shape[0]
    slots = places(me, False)
    copies = fill(stack.at[pl.ds(0, size), :], refs[:4], slots, sems.at[0])
    copies += fill(stack.at[pl.ds(size, size), :], refs[4:8], slots, sems.at[1])
    for copy in copies:
        copy.wait()
    band = lax.shift_right_logical(me, 2) * (4 * rows)

    def step(row, carry):
        for out, entry in ((low, rows), (high, (ITERS + 1) * rows)):
            source = (table[entry + row] - band) * 4
            move(out, as_index(row * 8, 8), stack, as_index(source, 4), 4)
            move(out, as_index(row * 8, 8) + 4, stack, size + source, 4)
        return carry

    lax.fori_loop(0, rows, step, 0, unroll=8)


def pick_half_kernel(rows, far, where, *refs):
    count = 2 if far else 1
    tables, sources, outs = refs[:count], refs[count : count + 4], refs[count + 4 : -2]
    stack, sems = refs[-2:]
    me = where[0]
    for copy in fill(stack, sources, places(me, far), sems):
        copy.wait()
    in_upper = lax.shift_right_logical(me, 2) ^ (1 if far else 0)
    band = in_upper * (4 * rows)
    entry = (in_upper * ITERS + 2) * rows

    def step(row, carry):
        for out, table in zip(outs, tables):
            source = (table[entry + row] - band) * 4
            move(out, as_index(row * 4, 4), stack, as_index(source, 4), 4)
        return carry

    lax.fori_loop(0, rows, step, 0, unroll=8)


def second_kernel(rows, where, counts, table, low, high, rim, first, second, extended):
    me = where[0]

    def gather(row, carry):
        move(extended, row * 16 + 12, rim, as_index(row * 4, 4), 4)
        move(extended, as_index(row * 16 + 16, 8), high, as_index(row * 8, 8), 8)
        return carry

    lax.fori_loop(0, rows, gather, 0, unroll=8)

    def lowered(row):
        return low[pl.ds(as_index(row * 8, 8), 8), :]

    add_delayed(rows, 1, table, live_limit(me, counts, 1, rows), extended, lowered, put_halves(first, second))


def last_kernel(rows, where, counts, table, low_a, low_b, high_a, high_b, rim_a, rim_b, merged, extended, low, lin):
    me = where[0]

    def gather(row, carry):
        for n, piece in enumerate((rim_a, rim_b, high_a, high_b)):
            move(extended, as_index(row * 16 + 8, 8) + n * 4, piece, as_index(row * 4, 4), 4)
        for n, piece in enumerate((low_a, low_b)):
            move(low, as_index(row * 8, 8) + n * 4, piece, as_index(row * 4, 4), 4)
        return carry

    lax.fori_loop(0, rows, gather, 0, unroll=8)

    def lowered(row):
        return low[pl.ds(as_index(row * 8, 8), 8), :]

    def put(row, total):
        lin[pl.ds(as_index(row * 8, 8), 8), :] = total

    add_delayed(rows, 2, table, live_limit(me, counts, 2, rows), extended, lowered, put)

    def step(group, carry):
        for piece in range(8):
            merged[pl.ds(as_index(group * 8, 8), 8), piece * LANES : (piece + 1) * LANES] = lin[
                pl.ds(group * 64 + piece, 8, stride=8), :
            ]
        return carry

    lax.fori_loop(0, rows // 8, step, 0, unroll=2)


SMEM = pl.BlockSpec(memory_space=pltpu.SMEM)
VMEM = pl.BlockSpec(memory_space=pltpu.VMEM)
HBM = pl.BlockSpec(memory_space=pl.ANY)


def f32(*shape):
    return jax.ShapeDtypeStruct(shape, jnp.float32)


def scratch(*shape):
    return pltpu.VMEM(shape, jnp.float32)


def call(kernel, ins, outs, scratches, *args):
    return pl.pallas_call(
        kernel,
        in_specs=list(ins),
        out_specs=[VMEM] * len(outs),
        out_shape=list(outs),
        scratch_shapes=list(scratches),
    )(*args)


def hop(block, pairs):
    return lax.ppermute(block, "freq", pairs)


def merged_by_chips(band_state, lower_rows, upper_rows, delays, counts):
    rows, samples = band_state.shape
    size = rows * (samples // LANES)
    half = size // 2
    devices = lax.axis_size("freq")
    steps = lax.axis_size("tm")
    me = lax.axis_index("freq").astype(jnp.int32)
    where = me[None]
    everyone = range(devices)
    hubs = [i for i in everyone if i & 2 != i >> 1 & 2]
    edges = [i for i in everyone if i not in hubs]

    def twist(block, bits):
        return hop(block, [(i, i ^ bits) for i in everyone])

    def onward(block):
        return lax.ppermute(block, "tm", [(t, t + 1) for t in range(steps - 1)])

    reach = rows // LANES
    lin, tail = call(
        partial(linear_kernel, reach), [VMEM], [f32(size, LANES), f32(rows * reach, LANES)], [], band_state
    )
    other = twist(lin, 1)
    grid = [(f, t) for f in everyone if f % 2 for t in range(steps - 1)]
    straight = [(f * steps + t, f * steps + t + 1) for f, t in grid]
    across = [(f * steps + t, (f - 1) * steps + t + 1) for f, t in grid]
    rim_odd = lax.ppermute(tail, ("freq", "tm"), straight)
    rim_even = lax.ppermute(tail, ("freq", "tm"), across)
    tables = jnp.concatenate([lower_rows, upper_rows, delays], axis=0)

    def own_table(device):
        return lax.dynamic_slice_in_dim(tables, device * rows, rows, axis=1).reshape(-1)

    table = own_table(me)
    table_over = own_table(me ^ 2)
    extended = scratch(rows * 16 + 16, LANES)
    halves = [f32(half, LANES)] * 2
    first, second = call(
        partial(first_kernel, rows),
        [SMEM] * 3 + [HBM] * 2 + [VMEM],
        halves,
        [scratch(2 * size, LANES), extended, pltpu.SemaphoreType.DMA((2,))],
        where, counts, table, lin, other, rim_odd + rim_even,
    )

    over_b = twist(second, 2)
    over_a = twist(first, 2)
    near_b = (second, twist(second, 1), over_b, twist(over_b, 1))
    stacked = [scratch(4 * half, LANES), pltpu.SemaphoreType.DMA((4,))]
    (rim,) = call(
        partial(pick_rim_kernel, rows), [SMEM] * 2 + [HBM] * 4, [f32(half, LANES)], stacked, where, table, *near_b
    )
    near_a = (first, twist(first, 1), over_a, twist(over_a, 1))
    rim = onward(rim)
    low, high = call(
        partial(pick_pair_kernel, rows),
        [SMEM] * 2 + [HBM] * 8,
        [f32(size, LANES)] * 2,
        [scratch(8 * half, LANES), pltpu.SemaphoreType.DMA((2, 4))],
        where, table, *near_a, *near_b,
    )
    first, second = call(
        partial(second_kernel, rows), [SMEM] * 3 + [VMEM] * 3, halves, [extended], where, counts, table, low, high, rim
    )

    hub = me & 2 != me >> 1 & 2
    in_upper = me >> 2 == 1

    def spread(block):
        inner = hop(block, [(i, i ^ 6) for i in hubs])
        outer = hop(block, [(i, i ^ 4) for i in edges])
        over = twist(block, 2)
        return block, inner, outer, over

    def selected(block, inner, outer, over):
        swapped = twist(inner, 1), twist(outer, 1)
        far_own, far_next = call(
            partial(pick_half_kernel, rows, True),
            [SMEM] * 3 + [HBM] * 4, halves, stacked,
            where, table, table_over, inner, swapped[0], outer, swapped[1],
        )
        handed = hop(far_next, [(i, i ^ 2) for i in hubs])
        swapped = twist(block, 1), twist(over, 1)
        (near,) = call(
            partial(pick_half_kernel, rows, False),
            [SMEM] * 2 + [HBM] * 4, [f32(half, LANES)], stacked,
            where, table, block, swapped[0], over, swapped[1],
        )
        return far_own, near, handed

    def arranged(far_own, near, handed):
        far = jnp.where(hub, far_own, handed)
        high = jnp.where(in_upper, near, far)
        low = jnp.where(in_upper, far, near)
        return low, high, onward(high)

    picked_b = selected(*spread(second))
    picked_a = selected(*spread(first))
    low_b, high_b, rim_b = arranged(*picked_b)
    low_a, high_a, rim_a = arranged(*picked_a)
    (merged,) = call(
        partial(last_kernel, rows),
        [SMEM] * 3 + [VMEM] * 6,
        [f32(rows, samples)],
        [extended, scratch(size, LANES), scratch(size, LANES)],
        where, counts, table, low_a, low_b, high_a, high_b, rim_a, rim_b,
    )
    return merged


def solution(mesh):
    def body(band_state, *tables):
        rows, samples = band_state.shape
        fits = rows == DMAX >> ITERS and rows % LANES == 0 and samples == 8 * LANES
        if ITERS == 3 and fits:
            return merged_by_chips(band_state, *tables)
        return per_device(band_state, *tables)

    return jax.shard_map(
        body,
        mesh=mesh,
        in_specs=(P("freq", "tm"), P(), P(), P(), P()),
        out_specs=P("freq", "tm"),
        check_vma=False,
    )
```
